256 devices in a mesh: lon: 16 (over x, y_hi, core), lat: 16 (over y_lo, z).
Axes of the slice: x: 4, y: 4 (y_hi: 2, y_lo: 2; y = y_hi * 2 + y_lo), z: 8, core: 2. Of those that a mesh axis runs over, the one named last changes fastest.
Arguments:
- grid_latent: bfloat16 [16, 16, 1024, 512], P('lat', 'lon'), may hold values from -6 to 6
- mesh_latent: bfloat16 [16, 16, 160, 512], P('lat', 'lon'), may hold values from -6 to 6
- edge_geometry: float32 [16, 16, 4, 2048], P('lat', 'lon'), may hold values from -6 to 6
- senders: int32 [16, 16, 2048], P('lat', 'lon'), may hold values from 0 to 1023
- receivers: int32 [16, 16, 2048], P('lat', 'lon'), may hold values from 0 to 1439, as said below
- w_grid: bfloat16 [512, 512], replicated, may hold values from -0.25 to 0.25
- w_mesh: bfloat16 [512, 512], replicated, may hold values from -0.25 to 0.25
- w_edge: float32 [4, 512], replicated, may hold values from -3 to 3
- edge_bias: float32 [512], replicated, may hold values from -3 to 3
- w_message: bfloat16 [512, 512], replicated, may hold values from -0.25 to 0.25
- w_node: bfloat16 [1024, 512], replicated, may hold values from -0.1875 to 0.1875
- w_output: bfloat16 [512, 512], replicated, may hold values from -0.25 to 0.25
- norm_gain: float32 [512], replicated, may hold values from 0.1 to 1.9
- norm_bias: float32 [512], replicated, may hold values from -3 to 3
Outputs:
- mesh_out: bfloat16 [16, 16, 160, 512], P('lat', 'lon')
The draws below stay inside these ranges and needn't reach their ends.
Inputs may be any that keep to these rules, and one draw needn't show every extreme that they name: `receivers`: r // 160 is a neighbour slot s from 0 to 8 (latitude offset s // 3 - 1, longitude offset s % 3 - 1); edges of the first band never name latitude offset -1, those of the last band never +1. For s other than 4, with k = s for s < 4 and k = s - 1 otherwise, the row r % 160 lies in k * 16 to k * 16 + 15 for s = 1, 3, 5, 7 and in k * 16 to k * 16 + 3 for s = 0, 2, 6, 8.
All inputs are finite; a program needn't handle non-finite values.
Results may differ from the reference program's by a relative error of at most 0.0095.
Values may be sent and summed in bfloat16 or wider, within the bound.
A program may use at most 64 MiB of HBM per device.

```python
import jax
import jax.numpy as jnp
from jax import lax

D = 512
M_DEV = 160
B_SIDE = 16
B_CORNER = 4
G_DEV = 1024
E_DEV = 2048
N_LON = 16
N_LAT = 16


def draw_receivers(key, part):
    base = jax.random.fold_in(key, 11)
    key_slot, key_side, key_corner, key_own = jax.random.split(base, 4)
    array_shape = (N_LAT, N_LON, E_DEV)
    raw_slot = jax.random.randint(key_slot, array_shape, 0, 40)
    neighbour = raw_slot - 32
    neighbour = neighbour + (neighbour >= 4).astype(jnp.int32)
    slot_number = jnp.where(raw_slot < 32, 4, neighbour)
    band_index = jnp.arange(N_LAT, dtype=jnp.int32)[:, None, None]
    lat_offset = slot_number // 3
    outside = (band_index == 0) & (lat_offset == 0) | (band_index == N_LAT - 1) & (lat_offset == 2)
    slot_number = jnp.where(outside, 3 + slot_number % 3, slot_number)
    side_row = jax.random.randint(key_side, array_shape, 0, B_SIDE)
    corner_row = jax.random.randint(key_corner, array_shape, 0, B_CORNER)
    own_row = jax.random.randint(key_own, array_shape, 0, M_DEV)
    strip_number = jnp.where(slot_number < 4, slot_number, slot_number - 1)
    is_corner = (slot_number % 2 == 0) & (slot_number != 4)
    border_row = strip_number * B_SIDE + jnp.where(is_corner, corner_row, side_row)
    row_number = jnp.where(slot_number == 4, own_row, border_row)
    return (slot_number * M_DEV + row_number).astype(jnp.int32)


def plant(drawn, own_key, least, high):
    place = [jax.random.randint(jax.random.fold_in(own_key, axis), (), 0, length) for axis, length in enumerate(drawn.shape)]
    main_axis = drawn.shape.index(max(drawn.shape))
    beside = place[:main_axis] + [(place[main_axis] + 1) % drawn.shape[main_axis]] + place[main_axis + 1:]
    return drawn.at[tuple(place)].set(least).at[tuple(beside)].set(high)


def levels(own_key, dims, cuts, least, top_value):
    level = 1.0
    for position, parts in cuts:
        draws = jax.random.uniform(jax.random.fold_in(jax.random.fold_in(own_key, 6), position), (parts,), jnp.float32, least / len(cuts), top_value / len(cuts))
        level = level * jnp.repeat(jnp.exp(draws), dims[position] // parts).reshape((-1,) + (1,) * (len(dims) - 1 - position))
    return level


def scatter_about(rng, extent, spread, bound, cuts=(), kind=jnp.bfloat16):
    level = levels(rng, extent, cuts, -0.22, 0.18) if cuts else 1.0
    result = jax.random.normal(rng, extent, jnp.float32) * spread * level
    return jnp.minimum(jnp.maximum(result, -bound), bound).astype(kind)


def setup_inputs(seed: int = 0) -> dict:
    seeds = jax.random.split(jax.random.key(seed), 15)
    return {
        "grid_latent": scatter_about(seeds[0], (N_LAT, N_LON, G_DEV, D), 1.0, 6.0, ((0, 16), (1, 16))),
        "mesh_latent": scatter_about(seeds[1], (N_LAT, N_LON, M_DEV, D), 1.0, 6.0, ((0, 16), (1, 16))),
        "edge_geometry": scatter_about(seeds[2], (N_LAT, N_LON, 4, E_DEV), 1.0, 6.0, ((0, 16), (1, 16)), jnp.float32),
        "senders": plant(jax.random.randint(seeds[3], (N_LAT, N_LON, E_DEV), 0, G_DEV), jax.random.fold_in(seeds[3], 1), 0, G_DEV - 1).astype(jnp.int32),
        "receivers": draw_receivers(jax.random.fold_in(seeds[14], 71), 0),
        "w_grid": scatter_about(seeds[5], (D, D), D ** -0.5, 0.25),
        "w_mesh": scatter_about(seeds[6], (D, D), D ** -0.5, 0.25),
        "w_edge": scatter_about(seeds[7], (4, D), 4 ** -0.5, 3.0, (), jnp.float32),
        "edge_bias": scatter_about(seeds[8], (D,), 0.5, 3.0, (), jnp.float32),
        "w_message": scatter_about(seeds[9], (D, D), D ** -0.5, 0.25),
        "w_node": scatter_about(seeds[10], (2 * D, D), (2 * D) ** -0.5, 0.1875),
        "w_output": scatter_about(seeds[11], (D, D), D ** -0.5, 0.25),
        "norm_gain": jnp.clip(1.0 + 0.18 * jax.random.normal(seeds[12], (D,), jnp.float32), 0.1, 1.9),
        "norm_bias": scatter_about(seeds[13], (D,), 0.5, 3.0, (), jnp.float32),
    }


def reference(grid_latent, mesh_latent, edge_geometry, senders, receivers, w_grid, w_mesh, w_edge, edge_bias, w_message, w_node, w_output, norm_gain, norm_bias):
    features = mesh_latent.shape[-1]
    mesh_flat = mesh_latent.reshape(-1, features)
    mesh_proj = jnp.dot(mesh_flat, w_mesh, preferred_element_type=jnp.float32)
    lon_index = jnp.arange(N_LON, dtype=jnp.int32)[:, None]

    def one_band(summed, items):
        band_grid, band_senders, band_receivers, band_geometry, band_index = items
        grid_proj = jnp.dot(band_grid.reshape(-1, features), w_grid, preferred_element_type=jnp.float32)
        grid_proj = grid_proj.reshape(N_LON, G_DEV, features)
        gathered = jax.vmap(lambda table, picks: jnp.take(table, picks, axis=0))(grid_proj, band_senders)
        slot_number = band_receivers // M_DEV
        row_number = band_receivers % M_DEV
        target_lat = band_index + slot_number // 3 - 1
        target_lon = (lon_index + slot_number % 3 - 1) % N_LON
        node_ids = ((target_lat * N_LON + target_lon) * M_DEV + row_number).astype(jnp.int32)
        geometry = jnp.einsum('lce,cd->led', band_geometry, w_edge, precision=lax.Precision.HIGHEST)
        preact = gathered + jnp.take(mesh_proj, node_ids, axis=0) + geometry + edge_bias
        hidden = jax.nn.silu(preact).astype(jnp.bfloat16)
        message = jnp.dot(hidden.reshape(-1, features), w_message, preferred_element_type=jnp.float32).astype(jnp.bfloat16)
        summed = summed + jax.ops.segment_sum(message.astype(jnp.float32), node_ids.reshape(-1), num_segments=mesh_flat.shape[0])
        return (summed, None)
    bands = jnp.arange(N_LAT, dtype=jnp.int32)
    start = jnp.zeros(mesh_flat.shape, jnp.float32)
    aggregated, _ = lax.scan(one_band, start, (grid_latent, senders, receivers, edge_geometry, bands))
    node_in = jnp.concatenate([mesh_flat, aggregated.astype(jnp.bfloat16)], axis=1)
    node_hidden = jax.nn.silu(jnp.dot(node_in, w_node, preferred_element_type=jnp.float32)).astype(jnp.bfloat16)
    update = jnp.dot(node_hidden, w_output, preferred_element_type=jnp.float32)
    row_mean = lax.optimization_barrier(jnp.mean(update, axis=-1, keepdims=True))
    centered = update - row_mean
    row_var = lax.optimization_barrier(jnp.mean(centered * centered, axis=-1, keepdims=True))
    normed = centered * lax.rsqrt(row_var + 1e-05) * norm_gain + norm_bias
    mesh_out = (mesh_flat.astype(jnp.float32) + normed).astype(jnp.bfloat16)
    return mesh_out.reshape(mesh_latent.shape)
```

```python
import functools

import jax
import jax.numpy as jnp
from jax import lax
from jax.experimental import pallas as pl
from jax.experimental.pallas import tpu as pltpu
from jax.sharding import PartitionSpec as P

B_SIDE = 16
BORDER = 8 * B_SIDE
EXTRA_AT = 160
BLOCK = 512
F32 = jnp.float32
BF16 = jnp.bfloat16
SLOTS = (0, 1, 2, 3, 5, 6, 7, 8)


def onehot(codes, picks):
    return jnp.where(codes == picks, jnp.ones((), BF16), jnp.zeros((), BF16))


def silu(x):
    half = 0.5 * x
    return half + half * jnp.tanh(half)


def dot(a, b):
    return jnp.dot(a, b, preferred_element_type=F32)


def dot_nt(a, b):
    return lax.dot_general(a, b, (((1,), (1,)), ((), ())), preferred_element_type=F32)


def pieces(x):
    first = x.astype(BF16).astype(F32)
    rest = x - first
    second = rest.astype(BF16).astype(F32)
    return first, second, rest - second


def kernel(
    n_lat,
    n_lon,
    grid_h,
    mesh_h,
    geo_h,
    snd_h,
    rcv_h,
    wg_h,
    wm_h,
    we_h,
    eb_h,
    wmsg_h,
    wnode_h,
    wout_h,
    gain_h,
    nb_h,
    out_ref,
    grid_v,
    mesh_v,
    geo_v,
    snd_v,
    rcv_v,
    wg_v,
    wm_v,
    we_v,
    eb_v,
    wmsg_v,
    wnode_v,
    wout_v,
    gain_v,
    nb_v,
    table_v,
    extra_v,
    gx_v,
    own_v,
    border_v,
    pre_v,
    hid_v,
    near_v,
    part_v,
    arrived_v,
    load_sem,
    send1,
    recv1,
    send2,
    recv2,
):
    lon = lax.axis_index("lon")
    lat = lax.axis_index("lat")
    rows = mesh_v.shape[0]
    features = mesh_v.shape[1]
    grid_rows = grid_v.shape[0]
    edges = snd_v.shape[1]

    def peer(slot, sign):
        up, right = slot // 3 - 1, slot % 3 - 1
        return {
            "lat": lax.rem(lat + sign * up + n_lat, n_lat),
            "lon": lax.rem(lon + sign * right + n_lon, n_lon),
        }

    barrier = pltpu.get_barrier_semaphore()
    for slot in SLOTS:
        pl.semaphore_signal(
            barrier, inc=1, device_id=peer(slot, 1), device_id_type=pl.DeviceIdType.MESH
        )
    loads = {}
    order = (
        ("mesh", mesh_h, mesh_v),
        ("wm", wm_h, wm_v),
        ("we", we_h, we_v),
        ("eb", eb_h, eb_v),
        ("geo", geo_h, geo_v),
        ("snd", snd_h, snd_v),
        ("rcv", rcv_h, rcv_v),
        ("wg", wg_h, wg_v),
        ("grid", grid_h, grid_v),
        ("wnode", wnode_h, wnode_v),
        ("wmsg", wmsg_h, wmsg_v),
        ("wout", wout_h, wout_v),
        ("gain", gain_h, gain_v),
        ("nb", nb_h, nb_v),
    )
    for number, (name, source, target) in enumerate(order):
        loads[name] = pltpu.make_async_copy(source, target, load_sem.at[number])
        loads[name].start()

    extra_v[...] = jnp.zeros_like(extra_v)
    gx_v[...] = jnp.zeros_like(gx_v)
    for name in ("mesh", "wm", "we", "eb", "geo", "snd", "rcv"):
        loads[name].wait()

    pl.semaphore_wait(barrier, len(SLOTS))
    first = []
    for k, slot in enumerate(SLOTS):
        part = pl.ds(k * B_SIDE, B_SIDE)
        copy = pltpu.make_async_remote_copy(
            src_ref=mesh_v.at[part],
            dst_ref=near_v.at[part],
            send_sem=send1.at[k],
            recv_sem=recv1.at[k],
            device_id=peer(slot, -1),
            device_id_type=pl.DeviceIdType.MESH,
        )
        copy.start()
        first.append(copy)

    w1, w2, w3 = pieces(we_v[...])
    g1, g2, g3 = pieces(geo_v[...])
    base = EXTRA_AT - 128
    for i, (g, w) in enumerate(((g1, w1), (g1, w2), (g2, w1), (g2, w2), (g1, w3), (g3, w1))):
        gx_v[4 * i : 4 * i + 4, :] = g
        extra_v[base + 4 * i : base + 4 * i + 4, :] = w
    gx_v[24:27, :] = jnp.ones((3, edges), F32)
    for i, b in enumerate(pieces(eb_v[...])):
        extra_v[base + 24 + i : base + 25 + i, :] = b

    wm_t = wm_v[...].T
    own_t = dot_nt(wm_t, mesh_v[...])
    own_t = jnp.concatenate(
        [own_t, jnp.zeros((features, 256 - rows), F32)], axis=1
    )
    own_t = own_t + jnp.concatenate([jnp.zeros((features, 128), F32), extra_v[...].T], axis=1)
    table_v[:, grid_rows : grid_rows + 256] = own_t.astype(BF16)

    loads["wg"].wait()
    loads["grid"].wait()
    wg_t = wg_v[...].T
    for at in range(0, grid_rows, 256):
        table_v[:, at : at + 256] = dot_nt(wg_t, grid_v[at : at + 256, :]).astype(BF16)

    i16 = jnp.int16
    grid_codes = lax.broadcasted_iota(jnp.int32, (grid_rows, BLOCK), 0).astype(i16)
    own_codes = (lax.broadcasted_iota(jnp.int32, (rows, BLOCK), 0) + 4 * rows).astype(i16)
    q = lax.broadcasted_iota(jnp.int32, (BORDER, BLOCK), 0)
    border_codes = (q + rows * ((q >> 4) + (q >= 64).astype(jnp.int32))).astype(i16)
    for at in range(0, edges, BLOCK):
        here = pl.ds(at, BLOCK)
        snd = snd_v[:, here].astype(i16)
        rcv = rcv_v[:, here].astype(i16)
        own = onehot(own_codes, rcv)
        own_v[:, here] = own
        border_v[:, here] = onehot(border_codes, rcv)
        stacked = jnp.concatenate(
            [
                onehot(grid_codes, snd),
                own,
                gx_v[:, here].astype(BF16),
                jnp.zeros((256 - rows - 32, BLOCK), BF16),
            ],
            axis=0,
        )
        pre_v[:, here] = dot(table_v[...], stacked)

    for copy in first:
        copy.wait_recv()
    near_t = dot_nt(wm_t, near_v[...]).astype(BF16)
    for at in range(0, edges, BLOCK):
        here = pl.ds(at, BLOCK)
        full = pre_v[:, here] + dot(near_t, border_v[:, here])
        hid_v[:, here] = silu(full).astype(BF16)
    part_v[...] = dot_nt(border_v[...], hid_v[...]).astype(BF16)

    second = []
    for k, slot in enumerate(SLOTS):
        part = pl.ds(k * B_SIDE, B_SIDE)
        copy = pltpu.make_async_remote_copy(
            src_ref=part_v.at[part],
            dst_ref=arrived_v.at[part],
            send_sem=send2.at[k],
            recv_sem=recv2.at[k],
            device_id=peer(slot, 1),
            device_id_type=pl.DeviceIdType.MESH,
        )
        copy.start()
        second.append(copy)

    own_sum = dot_nt(own_v[...], hid_v[...])
    for name in ("wnode", "wmsg", "wout", "gain", "nb"):
        loads[name].wait()
    node_pre = dot(mesh_v[...], wnode_v[0:features, :])
    for copy in first:
        copy.wait_send()
    for copy in second:
        copy.wait_recv()
    total = jnp.concatenate(
        [own_sum[:BORDER] + arrived_v[...].astype(F32), own_sum[BORDER:]], axis=0
    )
    high = total.astype(BF16)
    low = (total - high.astype(F32)).astype(BF16)
    summed = dot(high, wmsg_v[...]) + dot(low, wmsg_v[...])
    node_pre = node_pre + dot(summed.astype(BF16), wnode_v[features : 2 * features, :])
    update = dot(silu(node_pre).astype(BF16), wout_v[...])
    mean = jnp.mean(update, axis=-1, keepdims=True)
    centered = update - mean
    var = jnp.mean(centered * centered, axis=-1, keepdims=True)
    normed = centered * lax.rsqrt(var + 1e-05) * gain_v[...] + nb_v[...]
    out_ref[...] = (mesh_v[...].astype(F32) + normed).astype(BF16)
    for copy in second:
        copy.wait_send()


def solution(mesh):
    n_lat, n_lon = mesh.shape["lat"], mesh.shape["lon"]

    def local(
        grid_latent,
        mesh_latent,
        edge_geometry,
        senders,
        receivers,
        w_grid,
        w_mesh,
        w_edge,
        edge_bias,
        w_message,
        w_node,
        w_output,
        norm_gain,
        norm_bias,
    ):
        args = (
            grid_latent[0, 0],
            mesh_latent[0, 0],
            edge_geometry[0, 0],
            senders[0],
            receivers[0],
            w_grid,
            w_mesh,
            w_edge,
            edge_bias[None],
            w_message,
            w_node,
            w_output,
            norm_gain[None],
            norm_bias[None],
        )
        rows, features = args[1].shape
        edges = senders.shape[2]
        grid_rows = args[0].shape[0]
        out = pl.pallas_call(
            functools.partial(kernel, n_lat, n_lon),
            out_shape=jax.ShapeDtypeStruct((rows, features), BF16),
            in_specs=[pl.BlockSpec(memory_space=pl.ANY)] * len(args),
            out_specs=pl.BlockSpec(memory_space=pltpu.VMEM),
            scratch_shapes=[pltpu.VMEM(a.shape, a.dtype) for a in args]
            + [
                pltpu.VMEM((features, grid_rows + 256), BF16),
                pltpu.VMEM((128, features), F32),
                pltpu.VMEM((32, edges), F32),
                pltpu.VMEM((rows, edges), BF16),
                pltpu.VMEM((BORDER, edges), BF16),
                pltpu.VMEM((features, edges), F32),
                pltpu.VMEM((features, edges), BF16),
                pltpu.VMEM((BORDER, features), BF16),
                pltpu.VMEM((BORDER, features), BF16),
                pltpu.VMEM((BORDER, features), BF16),
                pltpu.SemaphoreType.DMA((len(args),)),
                pltpu.SemaphoreType.DMA((len(SLOTS),)),
                pltpu.SemaphoreType.DMA((len(SLOTS),)),
                pltpu.SemaphoreType.DMA((len(SLOTS),)),
                pltpu.SemaphoreType.DMA((len(SLOTS),)),
            ],
            compiler_params=pltpu.CompilerParams(
                collective_id=0, has_side_effects=True, vmem_limit_bytes=60 * 1024 * 1024
            ),
        )(*args)
        return out[None, None]

    return jax.shard_map(
        local,
        mesh=mesh,
        in_specs=(
            P("lat", "lon", None, None),
            P("lat", "lon", None, None),
            P("lat", "lon", None, None),
            P("lat", "lon", None),
            P("lat", "lon", None),
        )
        + (P(),) * 9,
        out_specs=P("lat", "lon", None, None),
        check_vma=False,
    )
```

```python
import functools

import jax
import jax.numpy as jnp
from jax import lax
from jax.experimental import pallas as pl
from jax.experimental.pallas import tpu as pltpu
from jax.sharding import PartitionSpec as P

B_SIDE = 16
BORDER = 8 * B_SIDE
BLOCK = 512
TAIL_BLOCK = 256
F32 = jnp.float32
BF16 = jnp.bfloat16
SLOTS = (3, 5, 0, 2, 6, 8, 1, 7)
CORNER_ROWS = 8


def onehot(codes, picks):
    return jnp.where(codes == picks, jnp.ones((), BF16), jnp.zeros((), BF16))


def silu(x):
    half = 0.5 * x
    return half + half * jnp.tanh(half)


def dot(a, b):
    return jnp.dot(a, b, preferred_element_type=F32)


def dot_nt(a, b):
    return lax.dot_general(a, b, (((1,), (1,)), ((), ())), preferred_element_type=F32)


def pieces(x):
    first = x.astype(BF16).astype(F32)
    rest = x - first
    second = rest.astype(BF16).astype(F32)
    return first, second, rest - second


def kernel(
    n_lat,
    n_lon,
    grid_h,
    mesh_h,
    geo_h,
    snd_h,
    rcv_h,
    wg_h,
    wm_h,
    we_h,
    eb_h,
    wmsg_h,
    wnode_h,
    wout_h,
    gain_h,
    nb_h,
    out_ref,
    grid_v,
    mesh_v,
    geo_v,
    snd_v,
    rcv_v,
    wg_v,
    wm_v,
    we_v,
    eb_v,
    wmsg_v,
    wnode_v,
    wout_v,
    gain_v,
    nb_v,
    table_v,
    extra_v,
    gx_v,
    own_v,
    border_v,
    pre_v,
    hid_v,
    proj_v,
    near_v,
    part_v,
    arrived_v,
    load_sem,
    send1,
    recv1,
    send2,
    recv2,
):
    lon = lax.axis_index("lon")
    lat = lax.axis_index("lat")
    rows = mesh_v.shape[0]
    features = mesh_v.shape[1]
    grid_rows = grid_v.shape[0]
    edges = snd_v.shape[1]
    mesh_ids = pl.DeviceIdType.MESH

    def peer(slot, sign):
        up, right = sign * (slot // 3 - 1), sign * (slot % 3 - 1)
        return {"lat": lat + up, "lon": lax.rem(lon + right + n_lon, n_lon)}

    def if_peer(slot, sign, action):
        up = sign * (slot // 3 - 1)
        if up == 0:
            action()
        elif up < 0:
            pl.when(lat > 0)(action)
        else:
            pl.when(lat < n_lat - 1)(action)

    def exchange(source, target, send_sem, recv_sem, sign):
        copies = []
        for slot in SLOTS:
            k = slot if slot < 4 else slot - 1
            part = pl.ds(k * B_SIDE, CORNER_ROWS if slot % 2 == 0 else B_SIDE)
            copies.append(
                pltpu.make_async_remote_copy(
                    src_ref=source.at[part],
                    dst_ref=target.at[part],
                    send_sem=send_sem.at[k],
                    recv_sem=recv_sem.at[k],
                    device_id=peer(slot, sign),
                    device_id_type=mesh_ids,
                )
            )
        return copies

    near_v[...] = jnp.zeros_like(near_v)
    arrived_v[...] = jnp.zeros_like(arrived_v)
    barrier = pltpu.get_barrier_semaphore()
    for slot in SLOTS:
        if_peer(
            slot,
            1,
            lambda: pl.semaphore_signal(
                barrier, inc=1, device_id=peer(slot, 1), device_id_type=mesh_ids
            ),
        )
    loads = {}
    order = (
        ("mesh", mesh_h, mesh_v),
        ("wm", wm_h, wm_v),
        ("we", we_h, we_v),
        ("eb", eb_h, eb_v),
        ("geo", geo_h, geo_v),
        ("snd", snd_h, snd_v),
        ("rcv", rcv_h, rcv_v),
        ("wg", wg_h, wg_v),
        ("grid", grid_h, grid_v),
        ("wnode", wnode_h, wnode_v),
        ("wmsg", wmsg_h, wmsg_v),
        ("wout", wout_h, wout_v),
        ("gain", gain_h, gain_v),
        ("nb", nb_h, nb_v),
    )
    for number, (name, source, target) in enumerate(order):
        loads[name] = pltpu.make_async_copy(source, target, load_sem.at[number])
        loads[name].start()
    extra_v[...] = jnp.zeros_like(extra_v)
    gx_v[...] = jnp.zeros_like(gx_v)
    for name in ("mesh", "wm"):
        loads[name].wait()
    proj_v[...] = dot(mesh_v[0:BORDER, :], wm_v[...]).astype(BF16)
    own_t = dot_nt(wm_v[...].T, mesh_v[...])
    for name in ("we", "eb", "geo", "snd", "rcv"):
        loads[name].wait()

    w1, w2, w3 = pieces(we_v[...])
    g1, g2, g3 = pieces(geo_v[...])
    base = rows - 128
    for i, (g, w) in enumerate(((g1, w1), (g1, w2), (g2, w1), (g2, w2), (g1, w3), (g3, w1))):
        gx_v[4 * i : 4 * i + 4, :] = g
        extra_v[base + 4 * i : base + 4 * i + 4, :] = w
    gx_v[24:27, :] = jnp.ones((3, edges), F32)
    for i, b in enumerate(pieces(eb_v[...])):
        extra_v[base + 24 + i : base + 25 + i, :] = b
    own_t = jnp.concatenate([own_t, jnp.zeros((features, 256 - rows), F32)], axis=1)
    own_t = own_t + jnp.concatenate([jnp.zeros((features, 128), F32), extra_v[...].T], axis=1)
    table_v[:, grid_rows : grid_rows + 256] = own_t.astype(BF16)
    ends = jnp.where(jnp.logical_or(lat == 0, lat == n_lat - 1), 3, 0)
    pl.semaphore_wait(barrier, len(SLOTS) - ends)
    first = exchange(proj_v, near_v, send1, recv1, -1)
    for slot, copy in zip(SLOTS, first):
        if_peer(slot, -1, copy.start)
    loads["wg"].wait()
    loads["grid"].wait()
    wg_t = wg_v[...].T
    for at in range(0, grid_rows, 256):
        table_v[:, at : at + 256] = dot_nt(wg_t, grid_v[at : at + 256, :]).astype(BF16)
    i16 = jnp.int16
    grid_codes = lax.broadcasted_iota(jnp.int32, (grid_rows, BLOCK), 0).astype(i16)
    own_codes = (lax.broadcasted_iota(jnp.int32, (rows, BLOCK), 0) + 4 * rows).astype(i16)
    q = lax.broadcasted_iota(jnp.int32, (BORDER, BLOCK), 0)
    border_codes = (q + rows * ((q >> 4) + (q >= 64).astype(jnp.int32))).astype(i16)
    for at in range(0, edges, BLOCK):
        here = pl.ds(at, BLOCK)
        snd = snd_v[:, here].astype(i16)
        rcv = rcv_v[:, here].astype(i16)
        own = onehot(own_codes, rcv)
        own_v[:, here] = own
        border_v[:, here] = onehot(border_codes, rcv)
        stacked = jnp.concatenate(
            [
                onehot(grid_codes, snd),
                own,
                gx_v[:, here].astype(BF16),
                jnp.zeros((256 - rows - 32, BLOCK), BF16),
            ],
            axis=0,
        )
        pre_v[:, here] = dot(table_v[...], stacked)
    for slot, copy in zip(SLOTS, first):
        if_peer(slot, 1, copy.wait_recv)
    near_t = near_v[...].T
    part_sum = jnp.zeros((BORDER, features), F32)
    ahead = dot(near_t, border_v[:, 0:TAIL_BLOCK])
    for at in range(0, edges, TAIL_BLOCK):
        here = pl.ds(at, TAIL_BLOCK)
        full = pre_v[:, here] + ahead
        if at + TAIL_BLOCK < edges:
            ahead = dot(near_t, border_v[:, at + TAIL_BLOCK : at + 2 * TAIL_BLOCK])
        hidden = silu(full).astype(BF16)
        hid_v[:, here] = hidden
        part_sum = part_sum + dot_nt(border_v[:, here], hidden)
    part_v[...] = part_sum.astype(BF16)
    second = exchange(part_v, arrived_v, send2, recv2, 1)
    for slot, copy in zip(SLOTS, second):
        if_peer(slot, 1, copy.start)
    own_sum = dot_nt(own_v[...], hid_v[...])
    for name in ("wnode", "wmsg", "wout", "gain", "nb"):
        loads[name].wait()
    joined = dot(wmsg_v[...], wnode_v[features : 2 * features, :]).astype(BF16)
    node_pre = dot(mesh_v[...], wnode_v[0:features, :])
    for slot, copy in zip(SLOTS, first):
        if_peer(slot, -1, copy.wait_send)
    for slot, copy in zip(SLOTS, second):
        if_peer(slot, -1, copy.wait_recv)
    total = jnp.concatenate(
        [own_sum[:BORDER] + arrived_v[...].astype(F32), own_sum[BORDER:]], axis=0
    )
    node_pre = node_pre + dot(total.astype(BF16), joined)
    update = dot(silu(node_pre).astype(BF16), wout_v[...])
    mean = jnp.mean(update, axis=-1, keepdims=True)
    centered = update - mean
    var = jnp.mean(centered * centered, axis=-1, keepdims=True)
    normed = centered * lax.rsqrt(var + 1e-05) * gain_v[...] + nb_v[...]
    out_ref[...] = (mesh_v[...].astype(F32) + normed).astype(BF16)
    for slot, copy in zip(SLOTS, second):
        if_peer(slot, 1, copy.wait_send)


def solution(mesh):
    n_lat, n_lon = mesh.shape["lat"], mesh.shape["lon"]

    def local(
        grid_latent,
        mesh_latent,
        edge_geometry,
        senders,
        receivers,
        w_grid,
        w_mesh,
        w_edge,
        edge_bias,
        w_message,
        w_node,
        w_output,
        norm_gain,
        norm_bias,
    ):
        args = (
            grid_latent[0, 0],
            mesh_latent[0, 0],
            edge_geometry[0, 0],
            senders[0],
            receivers[0],
            w_grid,
            w_mesh,
            w_edge,
            edge_bias[None],
            w_message,
            w_node,
            w_output,
            norm_gain[None],
            norm_bias[None],
        )
        rows, features = args[1].shape
        edges = senders.shape[2]
        grid_rows = args[0].shape[0]
        out = pl.pallas_call(
            functools.partial(kernel, n_lat, n_lon),
            out_shape=pltpu.VMEM((rows, features), BF16),
            in_specs=[pl.BlockSpec(memory_space=pl.ANY)] * len(args),
            out_specs=pl.BlockSpec(memory_space=pltpu.VMEM),
            scratch_shapes=[pltpu.VMEM(a.shape, a.dtype) for a in args]
            + [
                pltpu.VMEM((features, grid_rows + 256), BF16),
                pltpu.VMEM((128, features), F32),
                pltpu.VMEM((32, edges), F32),
                pltpu.VMEM((rows, edges), BF16),
                pltpu.VMEM((BORDER, edges), BF16),
                pltpu.VMEM((features, edges), F32),
                pltpu.VMEM((features, edges), BF16),
                pltpu.VMEM((BORDER, features), BF16),
                pltpu.VMEM((BORDER, features), BF16),
                pltpu.VMEM((BORDER, features), BF16),
                pltpu.VMEM((BORDER, features), BF16),
                pltpu.SemaphoreType.DMA((len(args),)),
                pltpu.SemaphoreType.DMA((len(SLOTS),)),
                pltpu.SemaphoreType.DMA((len(SLOTS),)),
                pltpu.SemaphoreType.DMA((len(SLOTS),)),
                pltpu.SemaphoreType.DMA((len(SLOTS),)),
            ],
            compiler_params=pltpu.CompilerParams(
                collective_id=0, has_side_effects=True, vmem_limit_bytes=60 * 1024 * 1024
            ),
        )(*args)
        return out[None, None]

    return jax.shard_map(
        local,
        mesh=mesh,
        in_specs=(
            P("lat", "lon", None, None),
            P("lat", "lon", None, None),
            P("lat", "lon", None, None),
            P("lat", "lon", None),
            P("lat", "lon", None),
        )
        + (P(),) * 9,
        out_specs=P("lat", "lon", None, None),
        check_vma=False,
    )
```

```python
import functools

import jax
import jax.numpy as jnp
from jax import lax
from jax.experimental import pallas as pl
from jax.experimental.pallas import tpu as pltpu
from jax.sharding import PartitionSpec as P

B_SIDE = 16
BORDER = 8 * B_SIDE
BLOCK = 512
TAIL_BLOCK = 512
F32 = jnp.float32
BF16 = jnp.bfloat16
SLOTS = (3, 5, 0, 2, 6, 8, 1, 7)
CORNER_ROWS = 8


def onehot(codes, picks):
    return jnp.where(codes == picks, jnp.ones((), BF16), jnp.zeros((), BF16))


def silu_of_double(half):
    return half + half * jnp.tanh(half)


def dot(a, b):
    return jnp.dot(a, b, preferred_element_type=F32)


def pieces(x):
    first = x.astype(BF16).astype(F32)
    rest = x - first
    second = rest.astype(BF16).astype(F32)
    return first, second, rest - second


def kernel(
    n_lat,
    n_lon,
    grid_h,
    mesh_h,
    geo_h,
    snd_h,
    rcv_h,
    wg_h,
    wm_h,
    we_h,
    eb_h,
    wmsg_h,
    wnode_h,
    wout_h,
    gain_h,
    nb_h,
    out_ref,
    grid_v,
    mesh_v,
    geo_v,
    snd_v,
    rcv_v,
    wg_v,
    wm_v,
    we_v,
    eb_v,
    wmsg_v,
    wnode_v,
    wout_v,
    gain_v,
    nb_v,
    table_v,
    extra_v,
    gx_v,
    own_v,
    border_v,
    pre_v,
    hid_v,
    near_pick_v,
    near_v,
    part_v,
    arrived_v,
    load_sem,
    send1,
    recv1,
    send2,
    recv2,
):
    lon = lax.axis_index("lon")
    lat = lax.axis_index("lat")
    rows = mesh_v.shape[0]
    features = mesh_v.shape[1]
    grid_rows = grid_v.shape[0]
    edges = geo_v.shape[1]
    mesh_ids = pl.DeviceIdType.MESH

    def peer(slot, sign):
        up, right = sign * (slot // 3 - 1), sign * (slot % 3 - 1)
        return {"lat": lat + up, "lon": lax.rem(lon + right + n_lon, n_lon)}

    def if_peer(slot, sign, action):
        up = sign * (slot // 3 - 1)
        if up == 0:
            action()
        elif up < 0:
            pl.when(lat > 0)(action)
        else:
            pl.when(lat < n_lat - 1)(action)

    def exchange(source, start, target, send_sem, recv_sem, sign):
        copies = []
        for slot in SLOTS:
            k = slot if slot < 4 else slot - 1
            count = CORNER_ROWS if slot % 2 == 0 else B_SIDE
            copies.append(
                pltpu.make_async_remote_copy(
                    src_ref=source.at[pl.ds(start + k * B_SIDE, count)],
                    dst_ref=target.at[pl.ds(k * B_SIDE, count)],
                    send_sem=send_sem.at[k],
                    recv_sem=recv_sem.at[k],
                    device_id=peer(slot, sign),
                    device_id_type=mesh_ids,
                )
            )
        return copies

    def clear(slots, first, count):
        for slot in slots:
            k = slot if slot < 4 else slot - 1
            here = pl.ds(k * B_SIDE + first, count)
            near_v[here, :] = jnp.zeros((count, features), BF16)
            arrived_v[here, :] = jnp.zeros((count, features), BF16)

    clear((0, 2, 6, 8), CORNER_ROWS, B_SIDE - CORNER_ROWS)
    pl.when(jnp.logical_or(lat == 0, lat == n_lat - 1))(
        lambda: clear((0, 1, 2, 6, 7, 8), 0, B_SIDE)
    )
    barrier = pltpu.get_barrier_semaphore()
    for slot in SLOTS:
        if_peer(
            slot,
            1,
            lambda: pl.semaphore_signal(
                barrier, inc=1, device_id=peer(slot, 1), device_id_type=mesh_ids
            ),
        )
    loads = {}
    order = (
        ("mesh", mesh_h, mesh_v),
        ("wm", wm_h, wm_v),
        ("we", we_h, we_v),
        ("eb", eb_h, eb_v),
        ("geo", geo_h, geo_v),
        ("snd", snd_h, snd_v),
        ("rcv", rcv_h, rcv_v),
        ("wg", wg_h, wg_v),
        ("grid", grid_h, grid_v),
        ("wnode", wnode_h, wnode_v),
        ("wmsg", wmsg_h, wmsg_v),
        ("wout", wout_h, wout_v),
        ("gain", gain_h, gain_v),
        ("nb", nb_h, nb_v),
    )
    for number, (name, source, target) in enumerate(order):
        loads[name] = pltpu.make_async_copy(source, target, load_sem.at[number])
        loads[name].start()
    extra_v[...] = jnp.zeros_like(extra_v)
    gx_v[...] = jnp.zeros_like(gx_v)
    for name in ("mesh", "wm"):
        loads[name].wait()
    own_at = pl.ds(grid_rows, rows)
    table_v[own_at, :] = (0.5 * dot(mesh_v[...], wm_v[...])).astype(BF16)
    loads["wg"].wait()
    loads["grid"].wait()
    for at in range(0, grid_rows, 512):
        table_v[at : at + 512, :] = (
            0.5 * dot(grid_v[at : at + 512, :], wg_v[...])
        ).astype(BF16)
    ends = jnp.where(jnp.logical_or(lat == 0, lat == n_lat - 1), 3, 0)
    pl.semaphore_wait(barrier, len(SLOTS) - ends)
    first = exchange(table_v, grid_rows, near_v, send1, recv1, -1)
    for slot, copy in zip(SLOTS, first):
        if_peer(slot, -1, copy.start)
    for name in ("we", "eb", "geo", "snd", "rcv"):
        loads[name].wait()
    w1, w2, w3 = pieces(we_v[...])
    g1, g2, g3 = pieces(geo_v[...])
    base = rows - 128
    for i, (g, w) in enumerate(((g1, w1), (g1, w2), (g2, w1), (g2, w2), (g1, w3), (g3, w1))):
        gx_v[base + 4 * i : base + 4 * i + 4, :] = g
        extra_v[4 * i : 4 * i + 4, :] = w
    gx_v[base + 24 : base + 27, :] = jnp.ones((3, edges), F32)
    for i, b in enumerate(pieces(eb_v[...])):
        extra_v[24 + i : 25 + i, :] = b
    table_v[grid_rows + rows :, :] = (0.5 * extra_v[...]).astype(BF16)
    i16 = jnp.int16
    snd_t = snd_v[...].T
    rcv_t = rcv_v[...].T
    lane = lax.broadcasted_iota(jnp.int32, (128, 128), 1)
    own_codes = (lax.broadcasted_iota(jnp.int32, (rows, 128), 0) + 4 * rows).astype(i16)
    q = lax.broadcasted_iota(jnp.int32, (BORDER, 128), 0)
    border_codes = (q + rows * ((q >> 4) + (q >= 64).astype(jnp.int32))).astype(i16)
    lane_codes = (lane + rows * ((lane >> 4) + (lane >= 64).astype(jnp.int32))).astype(i16)
    for at in range(0, edges, BLOCK):
        parts = []
        for c in range(at // 128, (at + BLOCK) // 128):
            here = pl.ds(c * 128, 128)
            snd = jnp.broadcast_to(snd_t[:, c : c + 1], (128, 128)).astype(i16)
            rcv = jnp.broadcast_to(rcv_t[:, c : c + 1], (128, 128)).astype(i16)
            near_pick_v[here, :] = onehot(lane_codes, rcv)
            rcv_row = rcv_v[c : c + 1, :].astype(i16)
            own_v[:, here] = onehot(own_codes, rcv_row)
            border_v[:, here] = onehot(border_codes, rcv_row)
            columns = [
                onehot((lane + t).astype(i16), snd) for t in range(0, grid_rows, 128)
            ]
            columns.append(onehot((lane + 4 * rows).astype(i16), rcv))
            tail = jnp.where(lane < rows - 128, lane + 4 * rows + 128, -1).astype(i16)
            columns.append(onehot(tail, rcv) + gx_v[:, here].astype(BF16).T)
            parts.append(jnp.concatenate(columns, axis=1))
        pre_v[pl.ds(at, BLOCK), :] = dot(jnp.concatenate(parts, axis=0), table_v[...])
    for slot, copy in zip(SLOTS, first):
        if_peer(slot, 1, copy.wait_recv)
    ahead = dot(near_pick_v[0:TAIL_BLOCK, :], near_v[...])
    for at in range(0, edges, TAIL_BLOCK):
        here = pl.ds(at, TAIL_BLOCK)
        full = pre_v[here, :] + ahead
        if at + TAIL_BLOCK < edges:
            ahead = dot(near_pick_v[at + TAIL_BLOCK : at + 2 * TAIL_BLOCK, :], near_v[...])
        hid_v[here, :] = silu_of_double(full).astype(BF16)
    part_v[...] = dot(border_v[...], hid_v[...]).astype(BF16)
    second = exchange(part_v, 0, arrived_v, send2, recv2, 1)
    for slot, copy in zip(SLOTS, second):
        if_peer(slot, 1, copy.start)
    own_sum = dot(own_v[...], hid_v[...])
    for name in ("wnode", "wmsg", "wout", "gain", "nb"):
        loads[name].wait()
    joined = dot(wmsg_v[...], wnode_v[features : 2 * features, :]).astype(BF16)
    node_pre = dot(mesh_v[...], wnode_v[0:features, :])
    for slot, copy in zip(SLOTS, first):
        if_peer(slot, -1, copy.wait_send)
    for slot, copy in zip(SLOTS, second):
        if_peer(slot, -1, copy.wait_recv)
    total = jnp.concatenate(
        [own_sum[:BORDER] + arrived_v[...].astype(F32), own_sum[BORDER:]], axis=0
    )
    node_pre = node_pre + dot(total.astype(BF16), joined)
    update = dot(silu_of_double(0.5 * node_pre).astype(BF16), wout_v[...])
    mean = jnp.mean(update, axis=-1, keepdims=True)
    centered = update - mean
    var = jnp.mean(centered * centered, axis=-1, keepdims=True)
    normed = centered * lax.rsqrt(var + 1e-05) * gain_v[...] + nb_v[...]
    out_ref[...] = (mesh_v[...].astype(F32) + normed).astype(BF16)
    for slot, copy in zip(SLOTS, second):
        if_peer(slot, 1, copy.wait_send)


def solution(mesh):
    n_lat, n_lon = mesh.shape["lat"], mesh.shape["lon"]

    def local(
        grid_latent,
        mesh_latent,
        edge_geometry,
        senders,
        receivers,
        w_grid,
        w_mesh,
        w_edge,
        edge_bias,
        w_message,
        w_node,
        w_output,
        norm_gain,
        norm_bias,
    ):
        args = (
            grid_latent[0, 0],
            mesh_latent[0, 0],
            edge_geometry[0, 0],
            senders[0, 0].reshape(-1, 128),
            receivers[0, 0].reshape(-1, 128),
            w_grid,
            w_mesh,
            w_edge,
            edge_bias[None],
            w_message,
            w_node,
            w_output,
            norm_gain[None],
            norm_bias[None],
        )
        rows, features = args[1].shape
        edges = senders.shape[2]
        grid_rows = args[0].shape[0]
        out = pl.pallas_call(
            functools.partial(kernel, n_lat, n_lon),
            out_shape=pltpu.VMEM((rows, features), BF16),
            in_specs=[pl.BlockSpec(memory_space=pl.ANY)] * len(args),
            out_specs=pl.BlockSpec(memory_space=pltpu.VMEM),
            scratch_shapes=[pltpu.VMEM(a.shape, a.dtype) for a in args]
            + [
                pltpu.VMEM((grid_rows + 256, features), BF16),
                pltpu.VMEM((256 - rows, features), F32),
                pltpu.VMEM((128, edges), F32),
                pltpu.VMEM((rows, edges), BF16),
                pltpu.VMEM((BORDER, edges), BF16),
                pltpu.VMEM((edges, features), F32),
                pltpu.VMEM((edges, features), BF16),
                pltpu.VMEM((edges, BORDER), BF16),
                pltpu.VMEM((BORDER, features), BF16),
                pltpu.VMEM((BORDER, features), BF16),
                pltpu.VMEM((BORDER, features), BF16),
                pltpu.SemaphoreType.DMA((len(args),)),
                pltpu.SemaphoreType.DMA((len(SLOTS),)),
                pltpu.SemaphoreType.DMA((len(SLOTS),)),
                pltpu.SemaphoreType.DMA((len(SLOTS),)),
                pltpu.SemaphoreType.DMA((len(SLOTS),)),
            ],
            compiler_params=pltpu.CompilerParams(
                collective_id=0, has_side_effects=True, vmem_limit_bytes=60 * 1024 * 1024
            ),
        )(*args)
        return out[None, None]

    return jax.shard_map(
        local,
        mesh=mesh,
        in_specs=(
            P("lat", "lon", None, None),
            P("lat", "lon", None, None),
            P("lat", "lon", None, None),
            P("lat", "lon", None),
            P("lat", "lon", None),
        )
        + (P(),) * 9,
        out_specs=P("lat", "lon", None, None),
        check_vma=False,
    )
```

```python
import functools

import jax
import jax.numpy as jnp
from jax import lax
from jax.experimental import pallas as pl
from jax.experimental.pallas import tpu as pltpu
from jax.sharding import PartitionSpec as P

B_SIDE = 16
BORDER = 8 * B_SIDE
BLOCK = 512
TAIL_BLOCK = 512
F32 = jnp.float32
BF16 = jnp.bfloat16
SLOTS = (2, 8, 5, 0, 6, 3, 1, 7)
CORNER_ROWS = 8
OUT, IN = 0, 1
ROUTES = ((0, OUT), (2, OUT), (1, OUT), (0, IN), (2, IN), (0, None), (2, None), (1, IN))
MESH = pl.DeviceIdType.MESH


def onehot(codes, picks):
    return jnp.where(codes == picks, jnp.ones((), BF16), jnp.zeros((), BF16))


def silu_of_double(half):
    return half + half * jnp.tanh(half)


def dot(a, b):
    return jnp.dot(a, b, preferred_element_type=F32)


def pieces(x):
    first = x.astype(BF16).astype(F32)
    rest = x - first
    second = rest.astype(BF16).astype(F32)
    return first, second, rest - second


def kernel(
    n_lat,
    n_lon,
    grid_h,
    mesh_h,
    geo_h,
    snd_h,
    rcv_h,
    wg_h,
    wm_h,
    we_h,
    eb_h,
    wmsg_h,
    wnode_h,
    wout_h,
    gain_h,
    nb_h,
    out_ref,
    grid_v,
    mesh_v,
    geo_v,
    snd_v,
    rcv_v,
    wg_v,
    wm_v,
    we_v,
    eb_v,
    wmsg_v,
    wnode_v,
    wout_v,
    gain_v,
    nb_v,
    table_v,
    extra_v,
    gx_v,
    own_v,
    border_v,
    pre_v,
    hid_v,
    near_pick_v,
    near_v,
    part_v,
    arrived_v,
    joined_v,
    centered_v,
    base_v,
    skip_v,
    load_sem,
    send_sem,
    relay_send_sem,
    near_sem,
    relay_sem,
    arrived_sem,
):
    lon = lax.axis_index("lon")
    lat = lax.axis_index("lat")
    rows = mesh_v.shape[0]
    features = mesh_v.shape[1]
    grid_rows = grid_v.shape[0]
    edges = geo_v.shape[1]

    first = lon == 0
    second = lon == 1
    last = lon == n_lon - 1
    at_end = jnp.logical_or(lat == 0, lat == n_lat - 1)
    inside = jnp.logical_not(at_end)

    def device(up, right):
        return {"lat": lat + up, "lon": lax.rem(lon + right + n_lon, n_lon)}

    def when(up, more, action):
        conditions = [] if more is None else [more]
        if up:
            conditions.append(lat > 0 if up < 0 else lat < n_lat - 1)
        if conditions:
            pl.when(functools.reduce(jnp.logical_and, conditions))(action)
        else:
            action()

    def signal(up, right):
        pl.semaphore_signal(barrier, inc=1, device_id=device(up, right), device_id_type=MESH)

    def send(source, start, target, at, count, sem, recv_sem, up, right):
        pltpu.make_async_remote_copy(
            src_ref=source.at[pl.ds(pl.multiple_of(start, B_SIDE), count)],
            dst_ref=target.at[pl.ds(pl.multiple_of(at, B_SIDE), count)],
            send_sem=sem.at[0],
            recv_sem=recv_sem.at[0],
            device_id=device(up, right),
            device_id_type=MESH,
        ).start()

    odd_lon = lax.rem(lon, 2)

    def strip(row, way, sign):
        if way is None:
            return 1 if row == 0 else 6, B_SIDE, 0
        right = 2 * odd_lon - 1 if way == OUT else 1 - 2 * odd_lon
        upper = odd_lon if (way == OUT) == (sign == 1) else 1 - odd_lon
        k = (2 * upper, 3 + upper, 5 + 2 * upper)[row]
        return k, B_SIDE if row == 1 else CORNER_ROWS, right

    def wait_rows(count, sem):
        here = hid_v.at[pl.ds(0, count)]
        pltpu.make_async_copy(here, here, sem).wait()

    def wait_strips(sem, all_rows, end_rows, more=None):
        for condition, count in ((inside, all_rows), (at_end, end_rows)):
            if more is not None:
                condition = jnp.logical_and(condition, more)
            pl.when(condition)(functools.partial(wait_rows, count, sem.at[0]))

    def clear(slots, first, count):
        for slot in slots:
            k = slot if slot < 4 else slot - 1
            here = pl.ds(k * B_SIDE + first, count)
            near_v[here, :] = jnp.zeros((count, features), BF16)
            arrived_v[here, :] = jnp.zeros((count, features), BF16)

    clear((0, 2, 6, 8), CORNER_ROWS, B_SIDE - CORNER_ROWS)
    pl.when(jnp.logical_or(lat == 0, lat == n_lat - 1))(
        lambda: clear((0, 1, 2, 6, 7, 8), 0, B_SIDE)
    )
    barrier = pltpu.get_barrier_semaphore()
    when(0, last, lambda: signal(0, 2))
    for slot in SLOTS:
        up, right = slot // 3 - 1, slot % 3 - 1
        more = jnp.logical_not(last) if right == 1 else None
        when(up, more, functools.partial(signal, up, right))
    order = (
        (0, mesh_h, mesh_v),
        (0, wm_h, wm_v),
        (2, wg_h, wg_v),
        (2, grid_h, grid_v),
        (1, we_h, we_v),
        (1, geo_h, geo_v),
        (1, snd_h, snd_v),
        (1, rcv_h, rcv_v),
        (4, eb_h, eb_v),
        (4, gain_h, gain_v),
        (4, nb_h, nb_v),
        (3, wnode_h, wnode_v),
        (3, wmsg_h, wmsg_v),
        (3, wout_h, wout_v),
    )
    totals = {}
    for number, source, target in order:
        pltpu.make_async_copy(source, target, load_sem.at[number]).start()
        totals[number] = totals.get(number, 0) + target.size * target.dtype.itemsize

    def loaded(number):
        wait_rows(totals[number] // (2 * features), load_sem.at[number])

    extra_v[...] = jnp.zeros_like(extra_v)
    gx_v[...] = jnp.zeros_like(gx_v)
    loaded(0)
    own_at = pl.ds(grid_rows, rows)
    table_v[own_at, :] = (0.5 * dot(mesh_v[...], wm_v[...])).astype(BF16)
    heard = jnp.where(at_end, 5, 8) + jnp.where(second, 1, 0)
    heard = heard - jnp.where(first, jnp.where(at_end, 2, 3), 0)
    pl.semaphore_wait(barrier, heard)
    def send_strips():
        for row, way in ROUTES:
            k, count, right = strip(row, way, -1)
            own = (table_v, grid_rows + k * B_SIDE, near_v)
            direct = functools.partial(
                send, *own, k * B_SIDE, count, send_sem, near_sem, 1 - row, right
            )
            if way == OUT:
                spot = BORDER + row * B_SIDE
                to_relay = functools.partial(
                    send, *own, spot, count, send_sem, relay_sem, 1 - row, 1
                )
                when(1 - row, jnp.logical_not(first), direct)
                when(1 - row, first, to_relay)
            else:
                when(1 - row, None, direct)

    strip_rows = 2 * CORNER_ROWS + B_SIDE

    def forward():
        wait_strips(relay_sem, strip_rows, strip_rows - CORNER_ROWS)
        for row, k, count in ((0, 2, CORNER_ROWS), (2, 7, CORNER_ROWS), (1, 4, B_SIDE)):
            from_row = BORDER + row * B_SIDE
            to = (near_v, k * B_SIDE, count, relay_send_sem, near_sem, 0, -2)
            when(row - 1, None, functools.partial(send, near_v, from_row, *to))
        send_strips()

    pl.when(jnp.logical_not(second))(send_strips)
    pl.when(second)(forward)
    loaded(1)
    vectors = hid_v.at[pl.ds(0, 8), pl.ds(0, totals[4] // 16)]
    pltpu.make_async_copy(vectors, vectors, load_sem.at[4]).wait()
    w1, w2, w3 = pieces(we_v[...])
    g1, g2, g3 = pieces(geo_v[...])
    base = rows - 128
    for i, (g, w) in enumerate(((g1, w1), (g1, w2), (g2, w1), (g2, w2), (g1, w3), (g3, w1))):
        gx_v[base + 4 * i : base + 4 * i + 4, :] = g
        extra_v[4 * i : 4 * i + 4, :] = w
    gx_v[base + 24 : base + 27, :] = jnp.ones((3, edges), F32)
    for i, b in enumerate(pieces(eb_v[...])):
        extra_v[24 + i : 25 + i, :] = b
    table_v[grid_rows + rows :, :] = (0.5 * extra_v[...]).astype(BF16)
    loaded(2)
    for at in range(0, grid_rows, 512):
        table_v[at : at + 512, :] = (
            0.5 * dot(grid_v[at : at + 512, :], wg_v[...])
        ).astype(BF16)
    i16 = jnp.int16
    snd_t = snd_v[...].T
    rcv_t = rcv_v[...].T
    lane = lax.broadcasted_iota(jnp.int32, (128, 128), 1)
    own_codes = (lax.broadcasted_iota(jnp.int32, (rows, 128), 0) + 4 * rows).astype(i16)
    q = lax.broadcasted_iota(jnp.int32, (BORDER, 128), 0)
    border_codes = (q + rows * ((q >> 4) + (q >= 64).astype(jnp.int32))).astype(i16)
    lane_codes = (lane + rows * ((lane >> 4) + (lane >= 64).astype(jnp.int32))).astype(i16)
    for at in range(0, edges, BLOCK):
        parts = []
        for c in range(at // 128, (at + BLOCK) // 128):
            here = pl.ds(c * 128, 128)
            snd = jnp.broadcast_to(snd_t[:, c : c + 1], (128, 128)).astype(i16)
            rcv = jnp.broadcast_to(rcv_t[:, c : c + 1], (128, 128)).astype(i16)
            near_pick_v[here, :] = onehot(lane_codes, rcv)
            rcv_row = rcv_v[c : c + 1, :].astype(i16)
            own_v[:, here] = onehot(own_codes, rcv_row)
            border_v[:, here] = onehot(border_codes, rcv_row)
            columns = [
                onehot((lane + t).astype(i16), snd) for t in range(0, grid_rows, 128)
            ]
            columns.append(onehot((lane + 4 * rows).astype(i16), rcv))
            tail = jnp.where(lane < rows - 128, lane + 4 * rows + 128, -1).astype(i16)
            columns.append(onehot(tail, rcv) + gx_v[:, here].astype(BF16).T)
            parts.append(jnp.concatenate(columns, axis=1))
        pre_v[pl.ds(at, BLOCK), :] = dot(jnp.concatenate(parts, axis=0), table_v[...])
    all_rows = 4 * (B_SIDE + CORNER_ROWS)
    wait_strips(near_sem, all_rows, all_rows - strip_rows)
    def strip_term(at):
        return dot(near_pick_v[at : at + TAIL_BLOCK, :], near_v[0:BORDER, :])

    terms = [strip_term(at) for at in range(0, 2 * TAIL_BLOCK, TAIL_BLOCK)]
    part_sum = None
    for at in range(0, edges, TAIL_BLOCK):
        here = pl.ds(at, TAIL_BLOCK)
        hid_v[here, :] = silu_of_double(pre_v[here, :] + terms.pop(0)).astype(BF16)
        later = at + 2 * TAIL_BLOCK
        if later < edges:
            terms.append(strip_term(later))
        done = at + TAIL_BLOCK
        if done % 512 == 0:
            add = dot(border_v[:, done - 512 : done], hid_v[done - 512 : done, :])
            part_sum = add if part_sum is None else part_sum + add
    part_v[...] = part_sum.astype(BF16)
    wait_strips(send_sem, all_rows, all_rows - strip_rows)
    for row, way in ROUTES:
        k, count, right = strip(row, way, 1)
        to = (arrived_v, k * B_SIDE, count, send_sem, arrived_sem, row - 1, right)
        when(row - 1, None, functools.partial(send, part_v, k * B_SIDE, *to))
    own_sum = dot(own_v[...], hid_v[...])
    loaded(3)
    joined_v[...] = (0.5 * dot(wmsg_v[...], wnode_v[features : 2 * features, :])).astype(BF16)
    base_v[...] = 0.5 * dot(mesh_v[...], wnode_v[0:features, :]) + dot(
        own_sum.astype(BF16), joined_v[...]
    )
    w_out = wout_v[...].astype(F32)
    centered_v[...] = (w_out - jnp.mean(w_out, axis=-1, keepdims=True)).astype(BF16)
    skip_v[...] = mesh_v[...].astype(F32) + nb_v[...]

    def node_layer(half, here):
        centered = dot(silu_of_double(half).astype(BF16), centered_v[...])
        var = jnp.mean(centered * centered, axis=-1, keepdims=True)
        normed = centered * lax.rsqrt(var + 1e-05) * gain_v[...]
        out_ref[here, :] = (skip_v[here, :] + normed).astype(BF16)

    inner = pl.ds(BORDER, rows - BORDER)
    node_layer(base_v[inner, :], inner)
    wait_strips(relay_send_sem, strip_rows, strip_rows - CORNER_ROWS, second)
    wait_strips(arrived_sem, all_rows, all_rows - strip_rows)
    strips = pl.ds(0, BORDER)
    node_layer(base_v[strips, :] + dot(arrived_v[...], joined_v[...]), strips)
    wait_strips(send_sem, all_rows, all_rows - strip_rows)


def solution(mesh):
    n_lat, n_lon = mesh.shape["lat"], mesh.shape["lon"]

    def local(
        grid_latent,
        mesh_latent,
        edge_geometry,
        senders,
        receivers,
        w_grid,
        w_mesh,
        w_edge,
        edge_bias,
        w_message,
        w_node,
        w_output,
        norm_gain,
        norm_bias,
    ):
        args = (
            grid_latent[0, 0],
            mesh_latent[0, 0],
            edge_geometry[0, 0],
            senders[0, 0].reshape(-1, 128),
            receivers[0, 0].reshape(-1, 128),
            w_grid,
            w_mesh,
            w_edge,
            edge_bias[None],
            w_message,
            w_node,
            w_output,
            norm_gain[None],
            norm_bias[None],
        )
        rows, features = args[1].shape
        edges = senders.shape[2]
        grid_rows = args[0].shape[0]
        out = pl.pallas_call(
            functools.partial(kernel, n_lat, n_lon),
            out_shape=pltpu.VMEM((rows, features), BF16),
            in_specs=[pl.BlockSpec(memory_space=pl.ANY)] * len(args),
            out_specs=pl.BlockSpec(memory_space=pltpu.VMEM),
            scratch_shapes=[pltpu.VMEM(a.shape, a.dtype) for a in args]
            + [
                pltpu.VMEM((grid_rows + 256, features), BF16),
                pltpu.VMEM((256 - rows, features), F32),
                pltpu.VMEM((128, edges), F32),
                pltpu.VMEM((rows, edges), BF16),
                pltpu.VMEM((BORDER, edges), BF16),
                pltpu.VMEM((edges, features), F32),
                pltpu.VMEM((edges, features), BF16),
                pltpu.VMEM((edges, BORDER), BF16),
                pltpu.VMEM((BORDER + 3 * B_SIDE, features), BF16),
                pltpu.VMEM((BORDER, features), BF16),
                pltpu.VMEM((BORDER, features), BF16),
                pltpu.VMEM((features, features), BF16),
                pltpu.VMEM((features, features), BF16),
                pltpu.VMEM((rows, features), F32),
                pltpu.VMEM((rows, features), F32),
                pltpu.SemaphoreType.DMA((5,)),
            ]
            + [pltpu.SemaphoreType.DMA((1,))] * 5,
            compiler_params=pltpu.CompilerParams(
                collective_id=0, has_side_effects=True, vmem_limit_bytes=60 * 1024 * 1024
            ),
        )(*args)
        return out[None, None]

    return jax.shard_map(
        local,
        mesh=mesh,
        in_specs=(
            P("lat", "lon", None, None),
            P("lat", "lon", None, None),
            P("lat", "lon", None, None),
            P("lat", "lon", None),
            P("lat", "lon", None),
        )
        + (P(),) * 9,
        out_specs=P("lat", "lon", None, None),
        check_vma=False,
    )
```
